32 devices in a mesh: groups: 2 (over y), ctx: 4 (over z), tp: 4 (over x, core).
Axes of the slice: x: 2, y: 2, z: 4, core: 2. Of those that a mesh axis runs over, the one named last changes fastest.
Arguments:
- q_nope: bfloat16 [512, 16384], P(('groups', 'ctx'), 'tp'), parts along dimension 0, may hold values from -6 to 6
- q_rope: bfloat16 [512, 8192], P(('groups', 'ctx'), 'tp'), parts along dimension 0, may hold values from -6 to 6
- c_kv: bfloat16 [512, 512], P(('groups', 'ctx')), parts along dimension 0, may hold values from -6 to 46.4
- k_rope: bfloat16 [512, 64], P(('groups', 'ctx')), parts along dimension 0, may hold values from -6 to 6
- positions: int32 [512], P(('groups', 'ctx')), parts along dimension 0, may hold values from 0 to 255, as said below
- w_uk: bfloat16 [128, 128, 512], P('tp', 'ctx'), may hold values from -0.5 to 0.5
- w_uv: bfloat16 [128, 512, 128], P('tp', 'ctx'), may hold values from -0.25 to 0.25
- w_out: bfloat16 [16384, 7168], P('tp', 'ctx'), may hold values from -0.125 to 0.125
Outputs:
- attn_proj: bfloat16 [512, 7168], P(('groups', 'tp'), 'ctx'), parts along dimension 0
The draws below stay inside these ranges and needn't reach their ends.
There are 2 independent parts, one for each index of `groups`. The reference program is written for one: setup_inputs(seed, part) draws one part's arguments, and reference() takes and returns one part's arrays. A program takes and returns all parts, laid end to end along the dimension named above; an argument that names none is the same for every part. Nothing has to cross between parts.
Inputs may be any that keep to these rules, and one draw needn't show every extreme that they name: The positions are the 256 integers 0 to 255, each once; every aligned block of 32 rows holds consecutive ascending positions.
All inputs are finite; a program needn't handle non-finite values.
Results may differ from the reference program's by a relative error of at most 0.015.
Values may be sent and summed in bfloat16 or wider, within the bound.
A program may use at most 64 MiB of HBM per device.

```python
import jax
import jax.numpy as jnp
from jax import lax

D = 7168
HEADS = 128
LAT = 512
ROPE = 64
NOPE = 128
VDIM = 128
TOK_DEV = 64
SEQ = 256


def draw_c_kv(key, part):
    latent = jnp.clip(jax.random.normal(key, (SEQ, LAT), jnp.float32), -6.0, 6.0)
    return latent.astype(jnp.bfloat16)


def draw_positions(key, part):
    half_len = TOK_DEV // 2
    block_count = SEQ // half_len
    order = jax.random.permutation(jax.random.fold_in(key, 11), block_count)
    grid = order[:, None].astype(jnp.int32) * half_len + jnp.arange(half_len, dtype=jnp.int32)[None, :]
    return grid.reshape(SEQ).astype(jnp.int32)


def block_scale(rng, dims, cuts, low, top_value):
    def one(dim, parts):
        draws = jax.random.uniform(jax.random.fold_in(jax.random.fold_in(rng, 6), dim), (parts,), jnp.float32, low / len(cuts), top_value / len(cuts))
        return jnp.repeat(jnp.exp(draws), dims[dim] // parts).reshape((-1,) + (1,) * (len(dims) - dim - 1))

    loudness = one(*cuts[0])
    for cut in cuts[1:]:
        loudness = loudness * one(*cut)
    return loudness


def scatter_about(key, shape, width, reach, pieces=(), kind=jnp.bfloat16):
    array = jax.random.normal(key, shape, jnp.float32) * width
    if len(pieces) > 0:
        array = block_scale(key, shape, pieces, -0.22, 0.18) * array
    return jnp.clip(array, min=-reach, max=reach).astype(kind)


def setup_inputs(seed: int = 0, part: int = 0) -> dict:
    splits = jax.random.split(jax.random.key(seed), 9)
    own_keys = jax.random.split(jax.random.fold_in(splits[8], part), 9)
    q_nope = scatter_about(own_keys[0], (SEQ, HEADS * NOPE), 1.0, 6.0, ((0, 4), (1, 4)))
    q_rope = scatter_about(own_keys[1], (SEQ, HEADS * ROPE), 1.0, 6.0, ((0, 4), (1, 4)))
    c_kv = draw_c_kv(jax.random.fold_in(jax.random.fold_in(splits[8], part), 71), part)
    k_rope = scatter_about(own_keys[3], (SEQ, ROPE), 1.0, 6.0, ((0, 4),))
    positions = draw_positions(jax.random.fold_in(jax.random.fold_in(splits[8], part), 71), part)
    w_uk = scatter_about(splits[5], (HEADS, NOPE, LAT), NOPE ** -0.5, 0.5, ((0, 4), (1, 4)))
    w_uv = scatter_about(splits[6], (HEADS, LAT, VDIM), LAT ** -0.5, 0.25, ((0, 4), (1, 4)))
    w_out = scatter_about(splits[7], (HEADS * VDIM, D), (HEADS * VDIM // 8) ** -0.5, 0.125, ((0, 4), (1, 4)))
    return {"q_nope": q_nope, "q_rope": q_rope, "c_kv": c_kv, "k_rope": k_rope, "positions": positions, "w_uk": w_uk, "w_uv": w_uv, "w_out": w_out}


def rotate(values, position):
    half_dim = values.shape[-1] // 2
    freqs = 10000.0 ** (-jnp.arange(half_dim, dtype=jnp.float32) / half_dim)
    angles = position.astype(jnp.float32)[..., None] * freqs
    cosine = jnp.cos(angles)
    sine = jnp.sin(angles)
    first_half = values[..., :half_dim].astype(jnp.float32)
    second_half = values[..., half_dim:].astype(jnp.float32)
    return jnp.concatenate([first_half * cosine - second_half * sine, second_half * cosine + first_half * sine], axis=-1)


def reference(q_nope, q_rope, c_kv, k_rope, positions, w_uk, w_uv, w_out):
    softmax_scale = (NOPE + ROPE) ** -0.5
    q_parts = q_nope.reshape(SEQ, HEADS, NOPE).astype(jnp.float32)
    q_lat = jnp.einsum("thn,hnl->htl", q_parts, w_uk.astype(jnp.float32)).astype(jnp.bfloat16)
    q_rot = rotate(q_rope.reshape(SEQ, HEADS, ROPE), positions[:, None]).astype(jnp.bfloat16)
    q_rot = jnp.transpose(q_rot, (1, 0, 2))
    k_rot = rotate(k_rope, positions).astype(jnp.bfloat16)
    key_rows = jnp.concatenate([c_kv, k_rot], axis=1)
    visible = positions[None, :] <= positions[:, None]

    def one_head(operands):
        lat_part, rot_part = operands
        queries = jnp.concatenate([lat_part, rot_part], axis=1)
        scores = jnp.dot(queries, key_rows.T, preferred_element_type=jnp.float32) * softmax_scale
        row_max = jnp.max(jnp.where(visible, scores, -1e30), axis=1)
        weights = jnp.where(visible, jnp.exp(scores - row_max[:, None]), 0.0)
        total = jnp.sum(weights, axis=1)
        mixed = jnp.dot(weights.astype(jnp.bfloat16), c_kv, preferred_element_type=jnp.float32)
        return (mixed / total[:, None]).astype(jnp.bfloat16)

    o_lat = lax.map(one_head, (q_lat, q_rot))
    head_out = jnp.einsum("hsl,hlv->shv", o_lat.astype(jnp.float32), w_uv.astype(jnp.float32))
    head_out = head_out.astype(jnp.bfloat16).reshape(SEQ, HEADS * VDIM)
    return jnp.dot(head_out, w_out, preferred_element_type=jnp.float32).astype(jnp.bfloat16)
```

```python
import functools

import jax
import jax.numpy as jnp
from jax import lax
from jax.experimental import pallas as pl
from jax.experimental.pallas import tpu as pltpu
from jax.sharding import PartitionSpec as P

F32 = jnp.float32
BF16 = jnp.bfloat16
MESH = pl.DeviceIdType.MESH


def rotate(values, position):
    half_dim = values.shape[-1] // 2
    freqs = 10000.0 ** (-jnp.arange(half_dim, dtype=jnp.float32) / half_dim)
    angles = position.astype(jnp.float32)[..., None] * freqs
    cosine = jnp.cos(angles)
    sine = jnp.sin(angles)
    first_half = values[..., :half_dim].astype(jnp.float32)
    second_half = values[..., half_dim:].astype(jnp.float32)
    return jnp.concatenate(
        [first_half * cosine - second_half * sine, second_half * cosine + first_half * sine],
        axis=-1,
    )


def rotate_flat(values, position, rope_dim):
    half_dim = rope_dim // 2
    copies = values.shape[1] // half_dim
    freqs = 10000.0 ** (-jnp.arange(half_dim, dtype=jnp.float32) / half_dim)
    angles = position.astype(jnp.float32)[:, None] * freqs
    cosine = jnp.tile(jnp.cos(angles), (1, copies))
    sine = jnp.tile(jnp.sin(angles), (1, copies))
    wide = values.astype(jnp.float32)
    lane = lax.broadcasted_iota(jnp.int32, wide.shape, 1)
    low = lax.rem(lane, rope_dim) < half_dim
    other = jnp.where(low, -jnp.roll(wide, -half_dim, axis=1), jnp.roll(wide, half_dim, axis=1))
    return wide * cosine + other * sine


def mega(sz, qn_in, qr_in, kv_in, wuk_in, wuv_in, wout_in, out_ref,
         qn, qr, kv, wuk, wuv, wout, krot, ho, acc, part, got,
         s1, r1, sy, ry, s_right, s_left, r_ag, s_rs, r_rs, loc, loc_out):
    n, groups, tps, nch = sz["n"], sz["g"], sz["t"], sz["nch"]
    tok, hpc, nope, rope, lat, vdim = (sz[k] for k in ("tok", "hpc", "nope", "rope", "lat", "vdim"))
    scale = (nope + rope) ** (-0.5)
    hc = hpc // nch
    hg = hc // groups
    c = lax.axis_index("ctx")
    g = lax.axis_index("groups")
    t = lax.axis_index("tp")
    nsl = nope // n
    lsl = lat // n

    barrier = pltpu.get_barrier_semaphore()
    for axis, me, count in (("ctx", c, n), ("groups", g, groups), ("tp", t, tps)):
        for d in range(1, count):
            pl.semaphore_signal(barrier, inc=1, device_id={axis: lax.rem(me + d, count)}, device_id_type=MESH)
    pl.semaphore_wait(barrier, (n - 1) + (groups - 1) + (tps - 1))

    def al(x, m):
        return pl.multiple_of(x, m)

    my_rows = pl.ds(al(c * tok, tok), tok)

    def rows_of(s):
        return pl.ds(al(s * tok, tok), tok)

    def piece(kind, i, j, s, gg):
        if kind == 0:
            return kv_in, kv.at[rows_of(s), :]
        if kind == 1:
            w = hc * nope
            return (qn_in.at[:, pl.ds(al(j * (hpc * nope) + i * w, w), w)],
                    qn.at[rows_of(s), pl.ds(i * w, w)])
        if kind == 2:
            w = hc * rope
            return (qr_in.at[:, pl.ds(al(j * (hpc * rope) + i * w, w), w)],
                    qr.at[rows_of(s), pl.ds(i * w, w)])
        if gg is None:
            src_h, dst_h = pl.ds(j * hpc + i * hc, hc), pl.ds(i * hc, hc)
        else:
            src_h, dst_h = pl.ds(j * hpc + i * hc + gg * hg, hg), pl.ds(i * hc + gg * hg, hg)
        if kind == 3:
            return wuk_in.at[src_h], wuk.at[dst_h, pl.ds(al(s * nsl, nsl), nsl), :]
        return wuv_in.at[src_h], wuv.at[dst_h, pl.ds(al(s * lsl, lsl), lsl), :]

    def copy1(kind, i, d, sending):
        if sending:
            j = lax.rem(c + d, n)
            src, dst = piece(kind, i, j, c, g)
        else:
            j = lax.rem(c + n - d, n)
            src, dst = piece(kind, i, c, j, g)
        return pltpu.make_async_remote_copy(
            src_ref=src, dst_ref=dst, send_sem=s1.at[kind, i, d - 1], recv_sem=r1.at[kind, i, d - 1],
            device_id={"ctx": j}, device_id_type=MESH)

    def local(kind, i):
        src, dst = piece(kind, i, c, c, None)
        return pltpu.make_async_copy(src, dst, loc.at[kind, i])

    def kinds(i):
        return (0, 1, 2, 3, 4) if i == 0 else (1, 2, 3, 4)

    for i in range(nch):
        for kind in (3, 4, 0, 1, 2):
            if kind in kinds(i):
                for d in range(n - 1, 0, -1):
                    copy1(kind, i, d, True).start()
    for i in range(nch):
        for kind in kinds(i):
            local(kind, i).start()
    wout_copy = pltpu.make_async_copy(wout_in, wout, loc_out)
    wout_copy.start()

    def copy_y(kind, i, e, d, sending):
        s = lax.rem(c + n - d, n)
        owner = g if sending else lax.rem(g + groups - e, groups)
        _, dst = piece(kind, i, c, s, owner)
        to = lax.rem(g + e, groups) if sending else owner
        return pltpu.make_async_remote_copy(
            src_ref=dst, dst_ref=dst, send_sem=sy.at[kind - 3, i, e - 1, d - 1],
            recv_sem=ry.at[kind - 3, i, e - 1, d - 1],
            device_id={"groups": to}, device_id_type=MESH)

    def forward_weights(i):
        for kind in (3, 4):
            for d in range(1, n):
                copy1(kind, i, d, False).wait_recv()
                for e in range(1, groups):
                    copy_y(kind, i, e, d, True).start()

    def ag_ref(i, b):
        return ho.at[b, i]

    def ag_copy(i, b, right):
        ref = ag_ref(i, b)
        return pltpu.make_async_remote_copy(
            src_ref=ref, dst_ref=ref, send_sem=(s_right if right else s_left).at[i, b],
            recv_sem=r_ag.at[i, b],
            device_id={"ctx": c + 1 if right else c - 1}, device_id_type=MESH)

    def attend(i):
        blk = kv[:, lat:lat + 2 * rope].astype(F32)
        lane = lax.broadcasted_iota(jnp.int32, blk.shape, 1)
        pos_col = jnp.sum(jnp.where(lane == rope, blk * 256.0, jnp.where(lane == rope + 1, blk, 0.0)),
                          axis=1, keepdims=True)
        blk_t = blk.T
        pos_row = blk_t[rope:rope + 1, :] * 256.0 + blk_t[rope + 1:rope + 2, :]
        hidden = pos_row > pos_col
        even = jnp.where(lane < rope, blk, 0.0)
        krot[0] = even.astype(BF16)
        krot[1] = pltpu.roll(even, rope, 1).astype(BF16)
        nt = (((1,), (1,)), ((), ()))

        def pair(p, carry):
            qrp = qr[:, pl.ds(al((i * (hc // 2) + p) * 2 * rope, 2 * rope), 2 * rope)]
            for k in range(2):
                hl = 2 * p + k
                h = i * hc + hl
                q = qn[:, pl.ds(al(h * nope, nope), nope)]
                ql = jnp.dot(q, wuk[h], preferred_element_type=F32).astype(BF16)
                sc = lax.dot_general(ql, kv[:, :lat], nt, preferred_element_type=F32)
                sc = (sc + lax.dot_general(qrp, krot[k], nt, preferred_element_type=F32)) * scale
                sc = jnp.where(hidden, -1e30, sc)
                w = jnp.exp(sc - jnp.max(sc, axis=1, keepdims=True))
                total = jnp.sum(w, axis=1, keepdims=True)
                o = jnp.dot(w.astype(BF16), kv[:, :lat], preferred_element_type=F32)
                o = (o / total).astype(BF16)
                ho[c, i, :, pl.ds(al(hl * vdim, vdim), vdim)] = jnp.dot(
                    o, wuv[h], preferred_element_type=F32).astype(BF16)
            return carry

        lax.fori_loop(0, hc // 2, pair, 0)

    for i in range(nch):
        if i == 0:
            forward_weights(0)
        for kind in (0, 1, 2):
            if kind in kinds(i):
                for d in range(1, n):
                    copy1(kind, i, d, False).wait_recv()
        for kind in kinds(i):
            local(kind, i).wait()
        for kind in (3, 4):
            for e in range(1, groups):
                for d in range(1, n):
                    copy_y(kind, i, e, d, False).wait_recv()
        if i + 1 < nch:
            forward_weights(i + 1)
        attend(i)

        @pl.when(c + 1 < n)
        def _():
            ag_copy(i, c, True).start()

        @pl.when(c > 0)
        def _():
            ag_copy(i, c, False).start()

    cols = acc.shape[1]
    tile = sz["tile"]
    kdim = hc * vdim

    def project(i, b, first):
        rows = pl.ds(al(b * (hpc * vdim) + i * kdim, kdim), kdim)

        def step(j, carry):
            at = pl.ds(al(j * tile, tile), tile)
            value = jnp.dot(ho[b, i], wout[rows, at], preferred_element_type=F32)
            acc[:, at] = value if first else acc[:, at] + value
            return carry

        lax.fori_loop(0, cols // tile, step, 0)

    wout_copy.wait()
    for i in range(nch):
        project(i, c, i == 0)
    for d in range(1, n):
        for i in range(nch):
            @pl.when(c - d >= 0)
            def _():
                b = c - d
                ag_copy(i, b, True).wait_recv()

                @pl.when(c + 1 < n)
                def _():
                    ag_copy(i, b, True).start()

            @pl.when(c + d < n)
            def _():
                b = c + d
                ag_copy(i, b, False).wait_recv()

                @pl.when(c > 0)
                def _():
                    ag_copy(i, b, False).start()

            @pl.when(c - d >= 0)
            def _():
                project(i, c - d, False)

            @pl.when(c + d < n)
            def _():
                project(i, c + d, False)

    rows_out = out_ref.shape[0]

    def rs_copy(d, sending):
        r = lax.rem(t + d, tps) if sending else lax.rem(t + tps - d, tps)
        return pltpu.make_async_remote_copy(
            src_ref=part.at[d - 1], dst_ref=got.at[d - 1], send_sem=s_rs.at[d - 1], recv_sem=r_rs.at[d - 1],
            device_id={"tp": r}, device_id_type=MESH)

    for d in range(1, tps):
        r = lax.rem(t + d, tps)
        part[d - 1] = acc[pl.ds(al(r * rows_out, rows_out), rows_out), :].astype(BF16)
        rs_copy(d, True).start()
    total = acc[pl.ds(al(t * rows_out, rows_out), rows_out), :]
    for d in range(1, tps):
        rs_copy(d, False).wait_recv()
        total = total + got[d - 1].astype(F32)
    out_ref[...] = total.astype(BF16)

    for i in range(nch):
        for kind in kinds(i):
            for d in range(1, n):
                copy1(kind, i, d, True).wait_send()
        for kind in (3, 4):
            for e in range(1, groups):
                for d in range(1, n):
                    copy_y(kind, i, e, d, True).wait_send()
        for b in range(n):
            @pl.when(jnp.logical_and(b <= c, c + 1 < n))
            def _():
                ag_copy(i, b, True).wait_send()

            @pl.when(jnp.logical_and(b >= c, c > 0))
            def _():
                ag_copy(i, b, False).wait_send()
    for d in range(1, tps):
        rs_copy(d, True).wait_send()


def fast(sz, q_nope, q_rope, c_kv, k_rope, positions, w_uk, w_uv, w_out):
    n, groups, tps, nch = sz["n"], sz["g"], sz["t"], sz["nch"]
    tok, hpc, nope, rope, lat, vdim = (sz[k] for k in ("tok", "hpc", "nope", "rope", "lat", "vdim"))
    hc = hpc // nch
    seq = n * tok
    cols = w_out.shape[1]
    q_rot = rotate_flat(q_rope, positions, rope).astype(BF16)
    k_rot = rotate(k_rope, positions).astype(BF16)
    high = (positions // 256).astype(BF16)[:, None]
    low = (positions % 256).astype(BF16)[:, None]
    key_rows = jnp.concatenate([c_kv, k_rot, high, low, jnp.zeros((tok, rope - 2), BF16)], axis=1)
    hbm = pl.BlockSpec(memory_space=pl.ANY)
    dma = pltpu.SemaphoreType.DMA
    return pl.pallas_call(
        functools.partial(mega, sz),
        out_shape=jax.ShapeDtypeStruct((seq // tps, cols), BF16),
        in_specs=[hbm] * 6,
        out_specs=pl.BlockSpec(memory_space=pltpu.VMEM),
        scratch_shapes=[
            pltpu.VMEM((seq, hpc * nope), BF16),
            pltpu.VMEM((seq, hpc * rope), BF16),
            pltpu.VMEM((seq, lat + 2 * rope), BF16),
            pltpu.VMEM((hpc, nope, lat), BF16),
            pltpu.VMEM((hpc, lat, vdim), BF16),
            pltpu.VMEM(w_out.shape, BF16),
            pltpu.VMEM((2, seq, 2 * rope), BF16),
            pltpu.VMEM((n, nch, seq, hc * vdim), BF16),
            pltpu.VMEM((seq, cols), F32),
            pltpu.VMEM((tps - 1, seq // tps, cols), BF16),
            pltpu.VMEM((tps - 1, seq // tps, cols), BF16),
            dma((5, nch, n - 1)),
            dma((5, nch, n - 1)),
            dma((2, nch, max(groups - 1, 1), n - 1)),
            dma((2, nch, max(groups - 1, 1), n - 1)),
            dma((nch, n)),
            dma((nch, n)),
            dma((nch, n)),
            dma((tps - 1,)),
            dma((tps - 1,)),
            dma((5, nch)),
            dma,
        ],
        compiler_params=pltpu.CompilerParams(collective_id=0, has_side_effects=True,
                                             vmem_limit_bytes=48 * 1024 * 1024),
    )(q_nope, q_rot, key_rows, w_uk, w_uv, w_out)


def general(q_nope, q_rope, c_kv, k_rope, positions, w_uk, w_uv, w_out):
    tok_count = q_nope.shape[0]
    head_count = w_uk.shape[0]
    latent = c_kv.shape[1]
    up_key, up_value = (
        lax.all_gather(w_uk, "ctx", axis=1, tiled=True),
        lax.all_gather(w_uv, "ctx", axis=1, tiled=True),
    )
    nope_dim = up_key.shape[1]
    rope_dim = k_rope.shape[1]
    softmax_scale = (nope_dim + rope_dim) ** (-0.5)
    q_parts = q_nope.reshape(tok_count, head_count, nope_dim)
    q_lat = jnp.einsum("thn,hnl->thl", q_parts, up_key, preferred_element_type=jnp.float32).astype(
        jnp.bfloat16
    )
    q_rot = rotate(q_rope.reshape(tok_count, head_count, rope_dim), positions[:, None]).astype(
        jnp.bfloat16
    )
    k_rot = rotate(k_rope, positions).astype(jnp.bfloat16)
    key_rows = jnp.concatenate([c_kv, k_rot], axis=1)
    queries = jnp.concatenate([q_lat, q_rot], axis=2).reshape(
        tok_count * head_count, latent + rope_dim
    )
    query_pos = jnp.repeat(positions, head_count)
    row_total = tok_count * head_count
    key_part = lax.all_gather(key_rows, "ctx", axis=0, tiled=True)
    key_pos = lax.all_gather(positions, "ctx", axis=0, tiled=True)
    run_max = jnp.full((row_total,), -1e30, jnp.float32)
    scores = (
        jnp.einsum("rk,sk->rs", queries, key_part, preferred_element_type=jnp.float32)
        * softmax_scale
    )
    visible = key_pos[None, :] <= query_pos[:, None]
    new_max = jnp.maximum(run_max, jnp.max(jnp.where(visible, scores, -1e30), axis=1))
    weights = jnp.where(visible, jnp.exp(scores - new_max[:, None]), 0.0)
    new_sum = jnp.sum(weights, axis=1)
    added = jnp.dot(
        weights.astype(jnp.bfloat16), key_part[:, :latent], preferred_element_type=jnp.float32
    )
    o_lat = (added / new_sum[:, None]).astype(jnp.bfloat16).reshape(tok_count, head_count, latent)
    head_out = jnp.einsum("thl,hlv->thv", o_lat, up_value, preferred_element_type=jnp.float32)
    rows_out = head_out.astype(jnp.bfloat16).reshape(tok_count, -1)
    partial_value = jnp.dot(
        lax.all_gather(rows_out, "ctx", axis=0, tiled=True),
        w_out,
        preferred_element_type=jnp.float32,
    )
    summed = lax.psum_scatter(
        partial_value.astype(jnp.bfloat16), "tp", scatter_dimension=0, tiled=True
    )
    return summed


CHUNKS = 2


def on_device(sizes, *args):
    q_nope, q_rope, c_kv, k_rope, positions, w_uk, w_uv, w_out = args
    n, groups, tps = sizes["ctx"], sizes["groups"], sizes["tp"]
    heads = w_uk.shape[0]
    hpc = heads // n
    sz = dict(n=n, g=groups, t=tps, nch=CHUNKS, tok=q_nope.shape[0], hpc=hpc,
              nope=w_uk.shape[1] * n, rope=k_rope.shape[1], lat=c_kv.shape[1],
              vdim=w_uv.shape[2], tile=256)
    seq = n * sz["tok"]
    cols = w_out.shape[1]
    fits = (
        heads % n == 0
        and n > 1
        and tps > 1
        and hpc % (CHUNKS * groups) == 0
        and (hpc // CHUNKS) % 2 == 0
        and seq <= 512
        and seq % (tps * 16) == 0
        and sz["tok"] % 16 == 0
        and sz["rope"] == 64
        and sz["nope"] % 128 == 0
        and sz["vdim"] % 128 == 0
        and sz["lat"] % 128 == 0
        and cols % 256 == 0
        and w_out.size * 2 + seq * cols * 8 <= 32 * 2**20
    )
    if fits:
        return fast(sz, *args)
    return general(*args)


def solution(mesh):
    in_specs = (
        P(("groups", "ctx"), "tp"),
        P(("groups", "ctx"), "tp"),
        P(("groups", "ctx"), None),
        P(("groups", "ctx"), None),
        P(("groups", "ctx")),
        P("tp", "ctx", None),
        P("tp", "ctx", None),
        P("tp", "ctx"),
    )
    out_specs = P(("groups", "tp"), "ctx")
    return jax.shard_map(
        functools.partial(on_device, dict(mesh.shape)),
        mesh=mesh, in_specs=in_specs, out_specs=out_specs, check_vma=False,
    )
```

```python
import functools
import math

import jax
import jax.numpy as jnp
from jax import lax
from jax.experimental import pallas as pl
from jax.experimental.pallas import tpu as pltpu
from jax.sharding import PartitionSpec as P

F32 = jnp.float32
BF16 = jnp.bfloat16
MESH = pl.DeviceIdType.MESH


def rotate(values, position):
    half_dim = values.shape[-1] // 2
    freqs = 10000.0 ** (-jnp.arange(half_dim, dtype=jnp.float32) / half_dim)
    angles = position.astype(jnp.float32)[..., None] * freqs
    cosine = jnp.cos(angles)
    sine = jnp.sin(angles)
    first_half = values[..., :half_dim].astype(jnp.float32)
    second_half = values[..., half_dim:].astype(jnp.float32)
    return jnp.concatenate(
        [first_half * cosine - second_half * sine, second_half * cosine + first_half * sine],
        axis=-1,
    )


def mega(sz, qn_in, qr_in, kv_in, kr_in, pos_in, wuk_in, wuv_in, wout_in, out_ref,
         qn, qr, kv, kr, pos, wuk, wuv, wout, krot, table, limit, ho, acc, part, got,
         s1, r1, sy, ry, st, rt, s_right, s_left, r_ag, s_rs, r_rs, loc, loc_out):
    n, groups, tps, nch = sz["n"], sz["g"], sz["t"], sz["nch"]
    tok, hpc, nope, rope, lat, vdim = (sz[k] for k in ("tok", "hpc", "nope", "rope", "lat", "vdim"))
    scale = (nope + rope) ** (-0.5)
    hc = hpc // nch
    hg = hc // groups
    c = lax.axis_index("ctx")
    g = lax.axis_index("groups")
    t = lax.axis_index("tp")
    nsl = nope // n
    lsl = lat // n
    share = tok // tps

    barrier = pltpu.get_barrier_semaphore()
    for axis, me, count in (("ctx", c, n), ("groups", g, groups), ("tp", t, tps)):
        for d in range(1, count):
            pl.semaphore_signal(barrier, inc=1, device_id={axis: lax.rem(me + d, count)}, device_id_type=MESH)
    pl.semaphore_wait(barrier, (n - 1) + (groups - 1) + (tps - 1))

    def al(x, m):
        return pl.multiple_of(x, m)

    def rows_of(s):
        return pl.ds(al(s * tok, tok), tok)

    def piece(kind, i, j, s, part_of):
        if kind in (0, 5):
            src, dst = (kv_in, kv) if kind == 0 else (kr_in, kr)
            if part_of is None:
                return src, dst.at[rows_of(s), :]
            return (src.at[pl.ds(al(part_of * share, share), share), :],
                    dst.at[pl.ds(al(s * tok + part_of * share, share), share), :])
        if kind == 6:
            return pos_in, pos.at[s]
        if kind == 1:
            w = hc * nope
            return (qn_in.at[:, pl.ds(al(j * (hpc * nope) + i * w, w), w)],
                    qn.at[rows_of(s), pl.ds(i * w, w)])
        if kind == 2:
            w = hc * rope
            return (qr_in.at[:, pl.ds(al(j * (hpc * rope) + i * w, w), w)],
                    qr.at[rows_of(s), pl.ds(i * w, w)])
        if part_of is None:
            src_h, dst_h = pl.ds(j * hpc + i * hc, hc), pl.ds(i * hc, hc)
        else:
            src_h = pl.ds(j * hpc + i * hc + part_of * hg, hg)
            dst_h = pl.ds(i * hc + part_of * hg, hg)
        if kind == 3:
            return wuk_in.at[src_h], wuk.at[dst_h, pl.ds(al(s * nsl, nsl), nsl), :]
        return wuv_in.at[src_h], wuv.at[dst_h, pl.ds(al(s * lsl, lsl), lsl), :]

    def copy1(kind, i, d, sending):
        mine = t if kind in (0, 5) else g
        if sending:
            j = lax.rem(c + d, n)
            src, dst = piece(kind, i, j, c, mine)
        else:
            j = lax.rem(c + n - d, n)
            src, dst = piece(kind, i, c, j, mine)
        return pltpu.make_async_remote_copy(
            src_ref=src, dst_ref=dst, send_sem=s1.at[kind, i, d - 1], recv_sem=r1.at[kind, i, d - 1],
            device_id={"ctx": j}, device_id_type=MESH)

    def local(kind, i):
        src, dst = piece(kind, i, c, c, None)
        return pltpu.make_async_copy(src, dst, loc.at[kind, i])

    def kinds(i):
        return (0, 1, 2, 3, 4, 5, 6) if i == 0 else (1, 2, 3, 4)

    order = [((6, 0, 5), 0), ((3, 4), 0)]
    for i in range(nch):
        if i + 1 < nch:
            order.append(((3, 4), i + 1))
        order.append(((1, 2), i))
    for group, i in order:
        for kind in group:
            for d in range(n - 1, 0, -1):
                copy1(kind, i, d, True).start()
    for i in range(nch):
        for kind in kinds(i):
            local(kind, i).start()
    wout_copy = pltpu.make_async_copy(wout_in, wout, loc_out)
    wout_copy.start()

    def copy_y(kind, i, e, d, sending):
        s = lax.rem(c + n - d, n)
        owner = g if sending else lax.rem(g + groups - e, groups)
        _, dst = piece(kind, i, c, s, owner)
        to = lax.rem(g + e, groups) if sending else owner
        return pltpu.make_async_remote_copy(
            src_ref=dst, dst_ref=dst, send_sem=sy.at[kind - 3, i, e - 1, d - 1],
            recv_sem=ry.at[kind - 3, i, e - 1, d - 1],
            device_id={"groups": to}, device_id_type=MESH)

    def copy_t(kind, e, d, sending):
        s = lax.rem(c + n - d, n)
        owner = t if sending else lax.rem(t + tps - e, tps)
        _, dst = piece(kind, 0, c, s, owner)
        to = lax.rem(t + e, tps) if sending else owner
        return pltpu.make_async_remote_copy(
            src_ref=dst, dst_ref=dst, send_sem=st.at[kind // 5, e - 1, d - 1],
            recv_sem=rt.at[kind // 5, e - 1, d - 1],
            device_id={"tp": to}, device_id_type=MESH)

    def forward_weights(i):
        for kind in (3, 4):
            for d in range(1, n):
                copy1(kind, i, d, False).wait_recv()
                for e in range(1, groups):
                    copy_y(kind, i, e, d, True).start()

    def forward_keys():
        for d in range(1, n):
            for kind in (0, 5):
                copy1(kind, 0, d, False).wait_recv()
                for e in range(1, tps):
                    copy_t(kind, e, d, True).start()

    def ag_copy(i, b, right):
        ref = ho.at[b, i]
        return pltpu.make_async_remote_copy(
            src_ref=ref, dst_ref=ref, send_sem=(s_right if right else s_left).at[i, b],
            recv_sem=r_ag.at[i, b],
            device_id={"ctx": c + 1 if right else c - 1}, device_id_type=MESH)

    wide = 2 * rope

    def turn(x):
        lane = lax.broadcasted_iota(jnp.int32, x.shape, 1)
        low = lax.rem(lane, rope) < rope // 2
        other = jnp.where(low, -pltpu.roll(x, wide - rope // 2, 1), pltpu.roll(x, rope // 2, 1))
        return x * table[0] + other * table[1]

    def tables():
        seq = n * tok
        for d in range(1, n):
            copy1(6, 0, d, False).wait_recv()
        local(6, 0).wait()
        row = jnp.concatenate([pos[s] for s in range(n)], axis=1).astype(F32)
        col = jnp.broadcast_to(row, (wide, seq)).T
        lane = lax.broadcasted_iota(jnp.int32, (1, wide), 1)
        index = lax.rem(lane, rope // 2).astype(F32)
        freqs = jnp.exp(index * (-math.log(10000.0) / (rope // 2)))
        angles = col * freqs
        table[0] = jnp.cos(angles)
        table[1] = jnp.sin(angles)
        limit[...] = jnp.where(row > col[:, :1], -1e30, 3e38)

    def keys():
        for kind in (0, 5):
            local(kind, 0).wait()
            for e in range(1, tps):
                for d in range(1, n):
                    copy_t(kind, e, d, False).wait_recv()
        raw = kr[...].astype(F32)
        turned = turn(jnp.concatenate([raw, raw], axis=1))
        lane = lax.broadcasted_iota(jnp.int32, turned.shape, 1)
        krot[0] = jnp.where(lane < rope, turned, 0.0).astype(BF16)
        krot[1] = jnp.where(lane < rope, 0.0, turned).astype(BF16)

    def attend(i):
        nt = (((1,), (1,)), ((), ()))

        def pair(p, carry):
            raw = qr[:, pl.ds(al((i * (hc // 2) + p) * wide, wide), wide)]
            qrp = turn(raw.astype(F32)).astype(BF16)
            for k in range(2):
                hl = 2 * p + k
                h = i * hc + hl
                q = qn[:, pl.ds(al(h * nope, nope), nope)]
                ql = jnp.dot(q, wuk[h], preferred_element_type=F32).astype(BF16)
                sc = lax.dot_general(ql, kv[...], nt, preferred_element_type=F32)
                sc = (sc + lax.dot_general(qrp, krot[k], nt, preferred_element_type=F32)) * scale
                sc = jnp.minimum(sc, limit[...])
                w = jnp.exp(sc - jnp.max(sc, axis=1, keepdims=True))
                total = jnp.sum(w, axis=1, keepdims=True)
                o = jnp.dot(w.astype(BF16), kv[...], preferred_element_type=F32)
                o = (o / total).astype(BF16)
                ho[c, i, :, pl.ds(al(hl * vdim, vdim), vdim)] = jnp.dot(
                    o, wuv[h], preferred_element_type=F32).astype(BF16)
            return carry

        lax.fori_loop(0, hc // 2, pair, 0)

    forward_keys()
    forward_weights(0)
    tables()
    keys()
    for i in range(nch):
        if i + 1 < nch:
            forward_weights(i + 1)
        for kind in (1, 2):
            for d in range(1, n):
                copy1(kind, i, d, False).wait_recv()
        for kind in (1, 2, 3, 4):
            local(kind, i).wait()
        for kind in (3, 4):
            for e in range(1, groups):
                for d in range(1, n):
                    copy_y(kind, i, e, d, False).wait_recv()
        attend(i)

        @pl.when(c + 1 < n)
        def _():
            ag_copy(i, c, True).start()

        @pl.when(c > 0)
        def _():
            ag_copy(i, c, False).start()

    cols = acc.shape[1]
    tile = sz["tile"]
    kdim = hc * vdim

    def project(i, b, first):
        rows = pl.ds(al(b * (hpc * vdim) + i * kdim, kdim), kdim)

        def step(j, carry):
            at = pl.ds(al(j * tile, tile), tile)
            value = jnp.dot(ho[b, i], wout[rows, at], preferred_element_type=F32)
            acc[:, at] = value if first else acc[:, at] + value
            return carry

        lax.fori_loop(0, cols // tile, step, 0)

    wout_copy.wait()
    for i in range(nch):
        project(i, c, i == 0)
    for d in range(1, n):
        for i in range(nch):
            @pl.when(c - d >= 0)
            def _():
                b = c - d
                ag_copy(i, b, True).wait_recv()

                @pl.when(c + 1 < n)
                def _():
                    ag_copy(i, b, True).start()

            @pl.when(c + d < n)
            def _():
                b = c + d
                ag_copy(i, b, False).wait_recv()

                @pl.when(c > 0)
                def _():
                    ag_copy(i, b, False).start()

            @pl.when(c - d >= 0)
            def _():
                project(i, c - d, False)

            @pl.when(c + d < n)
            def _():
                project(i, c + d, False)

    rows_out = out_ref.shape[0]

    def rs_copy(d, sending):
        r = lax.rem(t + d, tps) if sending else lax.rem(t + tps - d, tps)
        return pltpu.make_async_remote_copy(
            src_ref=part.at[d - 1], dst_ref=got.at[d - 1], send_sem=s_rs.at[d - 1], recv_sem=r_rs.at[d - 1],
            device_id={"tp": r}, device_id_type=MESH)

    for d in range(1, tps):
        r = lax.rem(t + d, tps)
        part[d - 1] = acc[pl.ds(al(r * rows_out, rows_out), rows_out), :].astype(BF16)
        rs_copy(d, True).start()
    total = acc[pl.ds(al(t * rows_out, rows_out), rows_out), :]
    for d in range(1, tps):
        rs_copy(d, False).wait_recv()
        total = total + got[d - 1].astype(F32)
    out_ref[...] = total.astype(BF16)

    for i in range(nch):
        for kind in kinds(i):
            for d in range(1, n):
                copy1(kind, i, d, True).wait_send()
        for kind in (3, 4):
            for e in range(1, groups):
                for d in range(1, n):
                    copy_y(kind, i, e, d, True).wait_send()
        for b in range(n):
            @pl.when(jnp.logical_and(b <= c, c + 1 < n))
            def _():
                ag_copy(i, b, True).wait_send()

            @pl.when(jnp.logical_and(b >= c, c > 0))
            def _():
                ag_copy(i, b, False).wait_send()
    for kind in (0, 5):
        for e in range(1, tps):
            for d in range(1, n):
                copy_t(kind, e, d, True).wait_send()
    for d in range(1, tps):
        rs_copy(d, True).wait_send()


def fast(sz, q_nope, q_rope, c_kv, k_rope, positions, w_uk, w_uv, w_out):
    n, groups, tps, nch = sz["n"], sz["g"], sz["t"], sz["nch"]
    tok, hpc, nope, rope, lat, vdim = (sz[k] for k in ("tok", "hpc", "nope", "rope", "lat", "vdim"))
    hc = hpc // nch
    seq = n * tok
    cols = w_out.shape[1]
    hbm = pl.BlockSpec(memory_space=pltpu.HBM)
    dma = pltpu.SemaphoreType.DMA
    more = max(groups - 1, 1)
    return pl.pallas_call(
        functools.partial(mega, sz),
        out_shape=jax.ShapeDtypeStruct((seq // tps, cols), BF16),
        in_specs=[hbm] * 8,
        out_specs=pl.BlockSpec(memory_space=pltpu.VMEM),
        scratch_shapes=[
            pltpu.VMEM((seq, hpc * nope), BF16),
            pltpu.VMEM((seq, hpc * rope), BF16),
            pltpu.VMEM((seq, lat), BF16),
            pltpu.VMEM((seq, rope), BF16),
            pltpu.VMEM((n, 1, tok), jnp.int32),
            pltpu.VMEM((hpc, nope, lat), BF16),
            pltpu.VMEM((hpc, lat, vdim), BF16),
            pltpu.VMEM(w_out.shape, BF16),
            pltpu.VMEM((2, seq, 2 * rope), BF16),
            pltpu.VMEM((2, seq, 2 * rope), F32),
            pltpu.VMEM((seq, seq), F32),
            pltpu.VMEM((n, nch, seq, hc * vdim), BF16),
            pltpu.VMEM((seq, cols), F32),
            pltpu.VMEM((tps - 1, seq // tps, cols), BF16),
            pltpu.VMEM((tps - 1, seq // tps, cols), BF16),
            dma((7, nch, n - 1)),
            dma((7, nch, n - 1)),
            dma((2, nch, more, n - 1)),
            dma((2, nch, more, n - 1)),
            dma((2, tps - 1, n - 1)),
            dma((2, tps - 1, n - 1)),
            dma((nch, n)),
            dma((nch, n)),
            dma((nch, n)),
            dma((tps - 1,)),
            dma((tps - 1,)),
            dma((7, nch)),
            dma,
        ],
        compiler_params=pltpu.CompilerParams(collective_id=0, has_side_effects=True,
                                             vmem_limit_bytes=60 * 1024 * 1024),
    )(q_nope, q_rope, c_kv, k_rope, positions.reshape(1, tok), w_uk, w_uv, w_out)


def general(q_nope, q_rope, c_kv, k_rope, positions, w_uk, w_uv, w_out):
    tok_count = q_nope.shape[0]
    head_count = w_uk.shape[0]
    latent = c_kv.shape[1]
    up_key, up_value = (
        lax.all_gather(w_uk, "ctx", axis=1, tiled=True),
        lax.all_gather(w_uv, "ctx", axis=1, tiled=True),
    )
    nope_dim = up_key.shape[1]
    rope_dim = k_rope.shape[1]
    softmax_scale = (nope_dim + rope_dim) ** (-0.5)
    q_parts = q_nope.reshape(tok_count, head_count, nope_dim)
    q_lat = jnp.einsum("thn,hnl->thl", q_parts, up_key, preferred_element_type=jnp.float32).astype(
        jnp.bfloat16
    )
    q_rot = rotate(q_rope.reshape(tok_count, head_count, rope_dim), positions[:, None]).astype(
        jnp.bfloat16
    )
    k_rot = rotate(k_rope, positions).astype(jnp.bfloat16)
    key_rows = jnp.concatenate([c_kv, k_rot], axis=1)
    queries = jnp.concatenate([q_lat, q_rot], axis=2).reshape(
        tok_count * head_count, latent + rope_dim
    )
    query_pos = jnp.repeat(positions, head_count)
    row_total = tok_count * head_count
    key_part = lax.all_gather(key_rows, "ctx", axis=0, tiled=True)
    key_pos = lax.all_gather(positions, "ctx", axis=0, tiled=True)
    run_max = jnp.full((row_total,), -1e30, jnp.float32)
    scores = (
        jnp.einsum("rk,sk->rs", queries, key_part, preferred_element_type=jnp.float32)
        * softmax_scale
    )
    visible = key_pos[None, :] <= query_pos[:, None]
    new_max = jnp.maximum(run_max, jnp.max(jnp.where(visible, scores, -1e30), axis=1))
    weights = jnp.where(visible, jnp.exp(scores - new_max[:, None]), 0.0)
    new_sum = jnp.sum(weights, axis=1)
    added = jnp.dot(
        weights.astype(jnp.bfloat16), key_part[:, :latent], preferred_element_type=jnp.float32
    )
    o_lat = (added / new_sum[:, None]).astype(jnp.bfloat16).reshape(tok_count, head_count, latent)
    head_out = jnp.einsum("thl,hlv->thv", o_lat, up_value, preferred_element_type=jnp.float32)
    rows_out = head_out.astype(jnp.bfloat16).reshape(tok_count, -1)
    partial_value = jnp.dot(
        lax.all_gather(rows_out, "ctx", axis=0, tiled=True),
        w_out,
        preferred_element_type=jnp.float32,
    )
    summed = lax.psum_scatter(
        partial_value.astype(jnp.bfloat16), "tp", scatter_dimension=0, tiled=True
    )
    return summed


CHUNKS = 4


def on_device(sizes, *args):
    q_nope, q_rope, c_kv, k_rope, positions, w_uk, w_uv, w_out = args
    n, groups, tps = sizes["ctx"], sizes["groups"], sizes["tp"]
    heads = w_uk.shape[0]
    hpc = heads // n
    sz = dict(n=n, g=groups, t=tps, nch=CHUNKS, tok=q_nope.shape[0], hpc=hpc,
              nope=w_uk.shape[1] * n, rope=k_rope.shape[1], lat=c_kv.shape[1],
              vdim=w_uv.shape[2], tile=256)
    seq = n * sz["tok"]
    cols = w_out.shape[1]
    fits = (
        heads % n == 0
        and n > 1
        and tps > 1
        and hpc % (CHUNKS * groups) == 0
        and (hpc // CHUNKS) % 2 == 0
        and seq <= 512
        and seq % (tps * 16) == 0
        and sz["tok"] % (tps * 16) == 0
        and sz["rope"] == 64
        and sz["nope"] % 128 == 0
        and sz["vdim"] % 128 == 0
        and sz["lat"] % 128 == 0
        and cols % 256 == 0
        and w_out.size * 2 + seq * cols * 8 <= 32 * 2**20
    )
    if fits:
        return fast(sz, *args)
    return general(*args)


def solution(mesh):
    in_specs = (
        P(("groups", "ctx"), "tp"),
        P(("groups", "ctx"), "tp"),
        P(("groups", "ctx"), None),
        P(("groups", "ctx"), None),
        P(("groups", "ctx")),
        P("tp", "ctx", None),
        P("tp", "ctx", None),
        P("tp", "ctx"),
    )
    out_specs = P(("groups", "tp"), "ctx")
    return jax.shard_map(
        functools.partial(on_device, dict(mesh.shape)),
        mesh=mesh, in_specs=in_specs, out_specs=out_specs, check_vma=False,
    )
```

```python
import functools
import math

import jax
import jax.numpy as jnp
from jax import lax
from jax.experimental import pallas as pl
from jax.experimental.pallas import tpu as pltpu
from jax.sharding import PartitionSpec as P

F32 = jnp.float32
BF16 = jnp.bfloat16
MESH = pl.DeviceIdType.MESH


def rotate(values, position):
    half_dim = values.shape[-1] // 2
    freqs = 10000.0 ** (-jnp.arange(half_dim, dtype=jnp.float32) / half_dim)
    angles = position.astype(jnp.float32)[..., None] * freqs
    cosine = jnp.cos(angles)
    sine = jnp.sin(angles)
    first_half = values[..., :half_dim].astype(jnp.float32)
    second_half = values[..., half_dim:].astype(jnp.float32)
    return jnp.concatenate(
        [first_half * cosine - second_half * sine, second_half * cosine + first_half * sine],
        axis=-1,
    )


def mega(sz, qn_in, qr_in, kv_in, kr_in, pos_in, wuk_in, wuv_in, wout_in, out_ref,
         qn, qr, kv, kr, pos, wuk, wuv, wout, krot, table, limit, ho, acc, part, got,
         s1, r1, sy, ry, st, rt, s_right, s_left, r_ag, s_rs, r_rs, loc, loc_out):
    n, groups, tps, nch = sz["n"], sz["g"], sz["t"], sz["nch"]
    tok, hpc, nope, rope, lat, vdim = (sz[k] for k in ("tok", "hpc", "nope", "rope", "lat", "vdim"))
    scale = (nope + rope) ** (-0.5)
    hc = hpc // nch
    hg = hc // groups
    c = lax.axis_index("ctx")
    g = lax.axis_index("groups")
    t = lax.axis_index("tp")
    nsl = nope // n
    lsl = lat // n
    share = tok // tps

    barrier = pltpu.get_barrier_semaphore()
    for axis, me, count in (("ctx", c, n), ("groups", g, groups), ("tp", t, tps)):
        for d in range(1, count):
            pl.semaphore_signal(barrier, inc=1, device_id={axis: lax.rem(me + d, count)}, device_id_type=MESH)
    pl.semaphore_wait(barrier, (n - 1) + (groups - 1) + (tps - 1))

    def al(x, m):
        return pl.multiple_of(x, m)

    def rows_of(s):
        return pl.ds(al(s * tok, tok), tok)

    def piece(kind, i, j, s, part_of):
        if kind in (0, 5):
            src, dst = (kv_in, kv) if kind == 0 else (kr_in, kr)
            if part_of is None:
                return src, dst.at[rows_of(s), :]
            return (src.at[pl.ds(al(part_of * share, share), share), :],
                    dst.at[pl.ds(al(s * tok + part_of * share, share), share), :])
        if kind == 6:
            return pos_in, pos.at[s]
        if kind == 1:
            w = hc * nope
            return (qn_in.at[:, pl.ds(al(j * (hpc * nope) + i * w, w), w)],
                    qn.at[rows_of(s), pl.ds(i * w, w)])
        if kind == 2:
            w = hc * rope
            return (qr_in.at[:, pl.ds(al(j * (hpc * rope) + i * w, w), w)],
                    qr.at[rows_of(s), pl.ds(i * w, w)])
        if part_of is None:
            src_h, dst_h = pl.ds(j * hpc + i * hc, hc), pl.ds(i * hc, hc)
        else:
            src_h = pl.ds(j * hpc + i * hc + part_of * hg, hg)
            dst_h = pl.ds(i * hc + part_of * hg, hg)
        if kind == 3:
            return wuk_in.at[src_h], wuk.at[dst_h, pl.ds(al(s * nsl, nsl), nsl), :]
        return wuv_in.at[src_h], wuv.at[dst_h, pl.ds(al(s * lsl, lsl), lsl), :]

    def copy1(kind, i, d, sending):
        mine = t if kind in (0, 5) else g
        if sending:
            j = lax.rem(c + d, n)
            src, dst = piece(kind, i, j, c, mine)
        else:
            j = lax.rem(c + n - d, n)
            src, dst = piece(kind, i, c, j, mine)
        return pltpu.make_async_remote_copy(
            src_ref=src, dst_ref=dst, send_sem=s1.at[kind, i, d - 1], recv_sem=r1.at[kind, i, d - 1],
            device_id={"ctx": j}, device_id_type=MESH)

    def local(kind, i):
        src, dst = piece(kind, i, c, c, None)
        return pltpu.make_async_copy(src, dst, loc.at[kind, i])

    def kinds(i):
        return (0, 1, 2, 3, 4, 5, 6) if i == 0 else (1, 2, 3, 4)

    order = [((6, 0, 5), 0), ((3, 4), 0)]
    for i in range(nch):
        if i + 1 < nch:
            order.append(((3, 4), i + 1))
        order.append(((1, 2), i))
    for group, i in order:
        for kind in group:
            for d in range(n - 1, 0, -1):
                copy1(kind, i, d, True).start()
    for i in range(nch):
        for kind in kinds(i):
            local(kind, i).start()
    wout_copy = pltpu.make_async_copy(wout_in, wout, loc_out)
    wout_copy.start()

    def copy_y(kind, i, e, d, sending):
        s = lax.rem(c + n - d, n)
        owner = g if sending else lax.rem(g + groups - e, groups)
        _, dst = piece(kind, i, c, s, owner)
        to = lax.rem(g + e, groups) if sending else owner
        return pltpu.make_async_remote_copy(
            src_ref=dst, dst_ref=dst, send_sem=sy.at[kind - 3, i, e - 1, d - 1],
            recv_sem=ry.at[kind - 3, i, e - 1, d - 1],
            device_id={"groups": to}, device_id_type=MESH)

    def copy_t(kind, e, d, sending):
        s = lax.rem(c + n - d, n)
        owner = t if sending else lax.rem(t + tps - e, tps)
        _, dst = piece(kind, 0, c, s, owner)
        to = lax.rem(t + e, tps) if sending else owner
        return pltpu.make_async_remote_copy(
            src_ref=dst, dst_ref=dst, send_sem=st.at[kind // 5, e - 1, d - 1],
            recv_sem=rt.at[kind // 5, e - 1, d - 1],
            device_id={"tp": to}, device_id_type=MESH)

    def forward_weights(i):
        for kind in (3, 4):
            for d in range(1, n):
                copy1(kind, i, d, False).wait_recv()
                for e in range(1, groups):
                    copy_y(kind, i, e, d, True).start()

    def forward_keys():
        for d in range(1, n):
            for kind in (0, 5):
                copy1(kind, 0, d, False).wait_recv()
                for e in range(1, tps):
                    copy_t(kind, e, d, True).start()

    def ag_copy(i, b, right):
        ref = ho.at[b, i]
        return pltpu.make_async_remote_copy(
            src_ref=ref, dst_ref=ref, send_sem=(s_right if right else s_left).at[i, b],
            recv_sem=r_ag.at[i, b],
            device_id={"ctx": c + 1 if right else c - 1}, device_id_type=MESH)

    wide = 2 * rope

    def turn(x):
        lane = lax.broadcasted_iota(jnp.int32, x.shape, 1)
        low = lax.rem(lane, rope) < rope // 2
        other = jnp.where(low, -pltpu.roll(x, wide - rope // 2, 1), pltpu.roll(x, rope // 2, 1))
        return x * table[0] + other * table[1]

    def tables():
        seq = n * tok
        for d in range(1, n):
            copy1(6, 0, d, False).wait_recv()
        local(6, 0).wait()
        row = jnp.concatenate([pos[s] for s in range(n)], axis=1).astype(F32)
        col = jnp.broadcast_to(row, (wide, seq)).T
        lane = lax.broadcasted_iota(jnp.int32, (1, wide), 1)
        index = lax.rem(lane, rope // 2).astype(F32)
        freqs = jnp.exp(index * (-math.log(10000.0) / (rope // 2)))
        angles = col * freqs
        table[0] = jnp.cos(angles)
        table[1] = jnp.sin(angles)
        limit[...] = jnp.where(row > col[:, :1], -1e30, 3e38)

    def keys():
        for kind in (0, 5):
            local(kind, 0).wait()
            for e in range(1, tps):
                for d in range(1, n):
                    copy_t(kind, e, d, False).wait_recv()
        raw = kr[...].astype(F32)
        turned = turn(jnp.concatenate([raw, raw], axis=1))
        lane = lax.broadcasted_iota(jnp.int32, turned.shape, 1)
        krot[0] = jnp.where(lane < rope, turned, 0.0).astype(BF16)
        krot[1] = jnp.where(lane < rope, 0.0, turned).astype(BF16)

    def attend(i):
        nt = (((1,), (1,)), ((), ()))

        def pair(p, carry):
            raw = qr[:, pl.ds(al((i * (hc // 2) + p) * wide, wide), wide)]
            qrp = turn(raw.astype(F32)).astype(BF16)
            for k in range(2):
                hl = 2 * p + k
                h = i * hc + hl
                q = qn[:, pl.ds(al(h * nope, nope), nope)]
                ql = jnp.dot(q, wuk[h], preferred_element_type=F32).astype(BF16)
                sc = lax.dot_general(ql, kv[...], nt, preferred_element_type=F32)
                sc = (sc + lax.dot_general(qrp, krot[k], nt, preferred_element_type=F32)) * scale
                sc = jnp.minimum(sc, limit[...])
                w = jnp.exp(sc - jnp.max(sc, axis=1, keepdims=True))
                total = jnp.sum(w, axis=1, keepdims=True)
                o = jnp.dot(w.astype(BF16), kv[...], preferred_element_type=F32)
                o = (o / total).astype(BF16)
                ho[c, i, :, pl.ds(al(hl * vdim, vdim), vdim)] = jnp.dot(
                    o, wuv[h], preferred_element_type=F32).astype(BF16)
            return carry

        lax.fori_loop(0, hc // 2, pair, 0)

    forward_keys()
    forward_weights(0)
    tables()
    keys()
    for i in range(nch):
        if i + 1 < nch:
            forward_weights(i + 1)
        for kind in (1, 2):
            for d in range(1, n):
                copy1(kind, i, d, False).wait_recv()
        for kind in (1, 2, 3, 4):
            local(kind, i).wait()
        for kind in (3, 4):
            for e in range(1, groups):
                for d in range(1, n):
                    copy_y(kind, i, e, d, False).wait_recv()
        attend(i)

        @pl.when(c + 1 < n)
        def _():
            ag_copy(i, c, True).start()

        @pl.when(c > 0)
        def _():
            ag_copy(i, c, False).start()

    cols = acc.shape[1]
    tile = sz["tile"]
    kdim = hc * vdim

    def project(i, b, first):
        rows = pl.ds(al(b * (hpc * vdim) + i * kdim, kdim), kdim)

        def step(j, carry):
            at = pl.ds(al(j * tile, tile), tile)
            value = jnp.dot(ho[b, i], wout[rows, at], preferred_element_type=F32)
            acc[:, at] = value if first else acc[:, at] + value
            return carry

        lax.fori_loop(0, cols // tile, step, 0)

    waited = False
    for d in range(1, n):
        for i in range(nch):
            @pl.when(c + d < n)
            def _():
                b = c + d
                ag_copy(i, b, False).wait_recv()

                @pl.when(c > 0)
                def _():
                    ag_copy(i, b, False).start()

            @pl.when(c - d >= 0)
            def _():
                b = c - d
                ag_copy(i, b, True).wait_recv()

                @pl.when(c + 1 < n)
                def _():
                    ag_copy(i, b, True).start()

            if not waited:
                wout_copy.wait()
                waited = True
            if d == 1:
                project(i, c, i == 0)

            @pl.when(c - d >= 0)
            def _():
                project(i, c - d, False)

            @pl.when(c + d < n)
            def _():
                project(i, c + d, False)

    rows_out = out_ref.shape[0]
    half = cols // 2
    core = lax.rem(t, 2)
    mate = t + 1 - 2 * core
    across = lax.rem(t + 2, tps)
    mate_across = lax.rem(mate + 2, tps)

    def block(r, at):
        return acc[pl.ds(al(r * rows_out, rows_out), rows_out), at]

    def rs_copy(stage, k):
        at = pl.ds(k * half, half)
        blocks = pl.ds(0, 2) if stage == 0 else pl.ds(2, 1)
        return pltpu.make_async_remote_copy(
            src_ref=part.at[blocks, :, at], dst_ref=got.at[blocks, :, at],
            send_sem=s_rs.at[stage, k], recv_sem=r_rs.at[stage, k],
            device_id={"tp": mate if stage == 0 else across}, device_id_type=MESH)

    spans = [slice(k * half, (k + 1) * half) for k in range(2)]
    for k, at in enumerate(spans):
        part[1, :, at] = block(mate_across, at).astype(BF16)
        part[0, :, at] = block(mate, at).astype(BF16)
        rs_copy(0, k).start()
    for k, at in enumerate(spans):
        rs_copy(0, k).wait_recv()
        part[2, :, at] = (block(across, at) + got[1, :, at].astype(F32)).astype(BF16)
        rs_copy(1, k).start()
    for k, at in enumerate(spans):
        own = block(t, at) + got[0, :, at].astype(F32)
        rs_copy(1, k).wait_recv()
        out_ref[:, at] = (own + got[2, :, at].astype(F32)).astype(BF16)

    for i in range(nch):
        for kind in kinds(i):
            for d in range(1, n):
                copy1(kind, i, d, True).wait_send()
        for kind in (3, 4):
            for e in range(1, groups):
                for d in range(1, n):
                    copy_y(kind, i, e, d, True).wait_send()
        for b in range(n):
            @pl.when(jnp.logical_and(b <= c, c + 1 < n))
            def _():
                ag_copy(i, b, True).wait_send()

            @pl.when(jnp.logical_and(b >= c, c > 0))
            def _():
                ag_copy(i, b, False).wait_send()
    for kind in (0, 5):
        for e in range(1, tps):
            for d in range(1, n):
                copy_t(kind, e, d, True).wait_send()
    for k in range(2):
        rs_copy(0, k).wait_send()
        rs_copy(1, k).wait_send()


def fast(sz, q_nope, q_rope, c_kv, k_rope, positions, w_uk, w_uv, w_out):
    n, groups, tps, nch = sz["n"], sz["g"], sz["t"], sz["nch"]
    tok, hpc, nope, rope, lat, vdim = (sz[k] for k in ("tok", "hpc", "nope", "rope", "lat", "vdim"))
    hc = hpc // nch
    seq = n * tok
    cols = w_out.shape[1]
    hbm = pl.BlockSpec(memory_space=pltpu.HBM)
    dma = pltpu.SemaphoreType.DMA
    more = max(groups - 1, 1)
    return pl.pallas_call(
        functools.partial(mega, sz),
        out_shape=jax.ShapeDtypeStruct((seq // tps, cols), BF16),
        in_specs=[hbm] * 8,
        out_specs=pl.BlockSpec(memory_space=pltpu.VMEM),
        scratch_shapes=[
            pltpu.VMEM((seq, hpc * nope), BF16),
            pltpu.VMEM((seq, hpc * rope), BF16),
            pltpu.VMEM((seq, lat), BF16),
            pltpu.VMEM((seq, rope), BF16),
            pltpu.VMEM((n, 1, tok), jnp.int32),
            pltpu.VMEM((hpc, nope, lat), BF16),
            pltpu.VMEM((hpc, lat, vdim), BF16),
            pltpu.VMEM(w_out.shape, BF16),
            pltpu.VMEM((2, seq, 2 * rope), BF16),
            pltpu.VMEM((2, seq, 2 * rope), F32),
            pltpu.VMEM((seq, seq), F32),
            pltpu.VMEM((n, nch, seq, hc * vdim), BF16),
            pltpu.VMEM((seq, cols), F32),
            pltpu.VMEM((tps - 1, seq // tps, cols), BF16),
            pltpu.VMEM((tps - 1, seq // tps, cols), BF16),
            dma((7, nch, n - 1)),
            dma((7, nch, n - 1)),
            dma((2, nch, more, n - 1)),
            dma((2, nch, more, n - 1)),
            dma((2, tps - 1, n - 1)),
            dma((2, tps - 1, n - 1)),
            dma((nch, n)),
            dma((nch, n)),
            dma((nch, n)),
            dma((2, 2)),
            dma((2, 2)),
            dma((7, nch)),
            dma,
        ],
        compiler_params=pltpu.CompilerParams(collective_id=0, has_side_effects=True,
                                             vmem_limit_bytes=60 * 1024 * 1024),
    )(q_nope, q_rope, c_kv, k_rope, positions.reshape(1, tok), w_uk, w_uv, w_out)


def general(q_nope, q_rope, c_kv, k_rope, positions, w_uk, w_uv, w_out):
    tok_count = q_nope.shape[0]
    head_count = w_uk.shape[0]
    latent = c_kv.shape[1]
    up_key, up_value = (
        lax.all_gather(w_uk, "ctx", axis=1, tiled=True),
        lax.all_gather(w_uv, "ctx", axis=1, tiled=True),
    )
    nope_dim = up_key.shape[1]
    rope_dim = k_rope.shape[1]
    softmax_scale = (nope_dim + rope_dim) ** (-0.5)
    q_parts = q_nope.reshape(tok_count, head_count, nope_dim)
    q_lat = jnp.einsum("thn,hnl->thl", q_parts, up_key, preferred_element_type=jnp.float32).astype(
        jnp.bfloat16
    )
    q_rot = rotate(q_rope.reshape(tok_count, head_count, rope_dim), positions[:, None]).astype(
        jnp.bfloat16
    )
    k_rot = rotate(k_rope, positions).astype(jnp.bfloat16)
    key_rows = jnp.concatenate([c_kv, k_rot], axis=1)
    queries = jnp.concatenate([q_lat, q_rot], axis=2).reshape(
        tok_count * head_count, latent + rope_dim
    )
    query_pos = jnp.repeat(positions, head_count)
    row_total = tok_count * head_count
    key_part = lax.all_gather(key_rows, "ctx", axis=0, tiled=True)
    key_pos = lax.all_gather(positions, "ctx", axis=0, tiled=True)
    run_max = jnp.full((row_total,), -1e30, jnp.float32)
    scores = (
        jnp.einsum("rk,sk->rs", queries, key_part, preferred_element_type=jnp.float32)
        * softmax_scale
    )
    visible = key_pos[None, :] <= query_pos[:, None]
    new_max = jnp.maximum(run_max, jnp.max(jnp.where(visible, scores, -1e30), axis=1))
    weights = jnp.where(visible, jnp.exp(scores - new_max[:, None]), 0.0)
    new_sum = jnp.sum(weights, axis=1)
    added = jnp.dot(
        weights.astype(jnp.bfloat16), key_part[:, :latent], preferred_element_type=jnp.float32
    )
    o_lat = (added / new_sum[:, None]).astype(jnp.bfloat16).reshape(tok_count, head_count, latent)
    head_out = jnp.einsum("thl,hlv->thv", o_lat, up_value, preferred_element_type=jnp.float32)
    rows_out = head_out.astype(jnp.bfloat16).reshape(tok_count, -1)
    partial_value = jnp.dot(
        lax.all_gather(rows_out, "ctx", axis=0, tiled=True),
        w_out,
        preferred_element_type=jnp.float32,
    )
    summed = lax.psum_scatter(
        partial_value.astype(jnp.bfloat16), "tp", scatter_dimension=0, tiled=True
    )
    return summed


CHUNKS = 4


def on_device(sizes, *args):
    q_nope, q_rope, c_kv, k_rope, positions, w_uk, w_uv, w_out = args
    n, groups, tps = sizes["ctx"], sizes["groups"], sizes["tp"]
    heads = w_uk.shape[0]
    hpc = heads // n
    sz = dict(n=n, g=groups, t=tps, nch=CHUNKS, tok=q_nope.shape[0], hpc=hpc,
              nope=w_uk.shape[1] * n, rope=k_rope.shape[1], lat=c_kv.shape[1],
              vdim=w_uv.shape[2], tile=w_out.shape[1] // 2)
    seq = n * sz["tok"]
    cols = w_out.shape[1]
    fits = (
        heads % n == 0
        and n > 1
        and tps == 4
        and hpc % (CHUNKS * groups) == 0
        and (hpc // CHUNKS) % 2 == 0
        and seq <= 512
        and seq % (tps * 16) == 0
        and sz["tok"] % (tps * 16) == 0
        and sz["rope"] == 64
        and sz["nope"] % 128 == 0
        and sz["vdim"] % 128 == 0
        and sz["lat"] % 128 == 0
        and cols % 256 == 0
        and w_out.size * 2 + seq * cols * 8 <= 32 * 2**20
    )
    if fits:
        return fast(sz, *args)
    return general(*args)


def solution(mesh):
    in_specs = (
        P(("groups", "ctx"), "tp"),
        P(("groups", "ctx"), "tp"),
        P(("groups", "ctx"), None),
        P(("groups", "ctx"), None),
        P(("groups", "ctx")),
        P("tp", "ctx", None),
        P("tp", "ctx", None),
        P("tp", "ctx"),
    )
    out_specs = P(("groups", "tp"), "ctx")
    return jax.shard_map(
        functools.partial(on_device, dict(mesh.shape)),
        mesh=mesh, in_specs=in_specs, out_specs=out_specs, check_vma=False,
    )
```
